32 devices in a mesh: gz: 8 (over z, x), gy: 4 (over y, core).
Axes of the slice: x: 2, y: 2, z: 4, core: 2. Of those that a mesh axis runs over, the one named last changes fastest.
Arguments:
- source_first: float32 [64, 32, 16, 128], P('gz', 'gy'), may hold values from -6 to 6
- source_second: float32 [32, 16, 16, 128], P('gz', 'gy'), may hold values from -6 to 6
- source_third: float32 [16, 8, 16, 128], P('gz', 'gy'), may hold values from -6 to 6
- source_fourth: float32 [8, 4, 16, 128], P('gz', 'gy'), may hold values from -6 to 6
- guess_first: float32 [64, 32, 16, 128], P('gz', 'gy'), may hold values from -6 to 6
- guess_second: float32 [32, 16, 16, 128], P('gz', 'gy'), may hold values from -6 to 6
- guess_third: float32 [16, 8, 16, 128], P('gz', 'gy'), may hold values from -6 to 6
- guess_fourth: float32 [8, 4, 16, 128], P('gz', 'gy'), may hold values from -6 to 6
- shift_first: float32 [64, 32, 128], P('gz', 'gy'), may hold values from 0.2 to 2
- shift_second: float32 [32, 16, 128], P('gz', 'gy'), may hold values from 0.2 to 2
- shift_third: float32 [16, 8, 128], P('gz', 'gy'), may hold values from 0.2 to 2
- shift_fourth: float32 [8, 4, 128], P('gz', 'gy'), may hold values from 0.2 to 2
- blocks_first: bfloat16 [64, 32, 2, 128, 128], P('gz', 'gy'), may hold values from -0.375 to 0.375
- blocks_second: bfloat16 [32, 16, 2, 128, 128], P('gz', 'gy'), may hold values from -0.375 to 0.375
- blocks_third: bfloat16 [16, 8, 2, 128, 128], P('gz', 'gy'), may hold values from -0.375 to 0.375
- links_first: int32 [64, 32, 2], P('gz', 'gy'), may hold values from 0 to 511, as said below
- links_second: int32 [32, 16, 2], P('gz', 'gy'), may hold values from 0 to 127, as said below
- links_third: int32 [16, 8, 2], P('gz', 'gy'), may hold values from 0 to 31, as said below
Outputs:
- smooth_first: float32 [64, 32, 16, 128], P('gz', 'gy')
- smooth_second: float32 [32, 16, 16, 128], P('gz', 'gy')
- smooth_third: float32 [16, 8, 16, 128], P('gz', 'gy')
- smooth_fourth: float32 [8, 4, 16, 128], P('gz', 'gy')
The draws below stay inside these ranges and needn't reach their ends.
Inputs may be any that keep to these rules, and one draw needn't show every extreme that they name: `links_first`: entry k of fine cell (i, j) names coarse column x * 16 + y with x within one of i // 2 and y within one of j // 2, both periodic on the coarse grid. `links_second`: entry k of cell (i, j) names coarse column x * 8 + y with x within one of i // 2 and y within one of j // 2, both periodic on the coarse grid. `links_third`: entry k of cell (i, j) names coarse column x * 4 + y with x within one of i // 2 and y within one of j // 2, both periodic on the coarse grid.
All inputs are finite; a program needn't handle non-finite values.
Results may differ from the reference program's by a relative error of at most 0.0005.
Values may be sent and summed in bfloat16 or wider, within the bound.
A program may use at most 256 MiB of HBM per device.

```python
import math
import jax
import jax.numpy as jnp
from jax import lax

LINE = 128
SIDES = 16
LINKS = 2
DEGREE = 3
NX0 = 64
NY0 = 32
NX1 = 32
NY1 = 16
NX2 = 16
NY2 = 8
NX3 = 8
NY3 = 4


def column_links(key, fine_rows, fine_cols, coarse_rows, coarse_cols):
    offsets = jax.random.randint(jax.random.fold_in(key, 17), (fine_rows, fine_cols, LINKS, 2), -1, 2)
    row_index = (jnp.arange(fine_rows, dtype=jnp.int32) // 2)[:, None, None]
    col_index = (jnp.arange(fine_cols, dtype=jnp.int32) // 2)[None, :, None]
    coarse_row = (row_index + offsets[..., 0]) % coarse_rows
    coarse_col = (col_index + offsets[..., 1]) % coarse_cols
    return (coarse_row * coarse_cols + coarse_col).astype(jnp.int32)


def draw_links_first(key, part):
    return column_links(key, NX0, NY0, NX1, NY1)


def draw_links_second(key, part):
    return column_links(key, NX1, NY1, NX2, NY2)


def draw_links_third(key, part):
    return column_links(key, NX2, NY2, NX3, NY3)


def level_of(own_key, extent, shards, low, high):
    loudness = 1.0
    for position, shards_of in shards:
        draws = jax.random.uniform(jax.random.fold_in(jax.random.fold_in(own_key, 6), position), (shards_of,), jnp.float32, low / len(shards), high / len(shards))
        loudness = loudness * jnp.repeat(jnp.exp(draws), extent[position] // shards_of).reshape((-1,) + (1,) * (len(extent) - 1 - position))
    return loudness


def centred(key, shape, width, most, shards=(), held_as=jnp.bfloat16):
    factor_of = level_of(key, shape, shards, -0.22, 0.18) if shards else 1.0
    array = jax.random.normal(key, shape, jnp.float32) * width * factor_of
    return jnp.minimum(jnp.maximum(array, -most), most).astype(held_as)


def setup_inputs(seed: int = 0) -> dict:
    key_list = jax.random.split(jax.random.key(seed), 19)
    source_first = centred(key_list[0], (NX0, NY0, SIDES, LINE), 1.0, 6.0, ((0, 8), (1, 4)), jnp.float32)
    source_second = centred(key_list[1], (NX1, NY1, SIDES, LINE), 1.0, 6.0, ((0, 8), (1, 4)), jnp.float32)
    source_third = centred(key_list[2], (NX2, NY2, SIDES, LINE), 1.0, 6.0, ((0, 8), (1, 4)), jnp.float32)
    source_fourth = centred(key_list[3], (NX3, NY3, SIDES, LINE), 1.0, 6.0, ((0, 8), (1, 4)), jnp.float32)
    guess_first = centred(key_list[4], (NX0, NY0, SIDES, LINE), 1.0, 6.0, ((0, 8), (1, 4)), jnp.float32)
    guess_second = centred(key_list[5], (NX1, NY1, SIDES, LINE), 1.0, 6.0, ((0, 8), (1, 4)), jnp.float32)
    guess_third = centred(key_list[6], (NX2, NY2, SIDES, LINE), 1.0, 6.0, ((0, 8), (1, 4)), jnp.float32)
    guess_fourth = centred(key_list[7], (NX3, NY3, SIDES, LINE), 1.0, 6.0, ((0, 8), (1, 4)), jnp.float32)
    shift_first = jnp.clip(jnp.exp(math.log(2.0) - 2.3025851 * jax.random.uniform(key_list[8], (NX0, NY0, LINE), jnp.float32) ** level_of(key_list[8], (NX0, NY0, LINE), ((0, 8), (1, 4)), -0.2, 0.2)), 0.2, 2.0)
    shift_second = jnp.clip(jnp.exp(math.log(2.0) - 2.3025851 * jax.random.uniform(key_list[9], (NX1, NY1, LINE), jnp.float32) ** level_of(key_list[9], (NX1, NY1, LINE), ((0, 8), (1, 4)), -0.2, 0.2)), 0.2, 2.0)
    shift_third = jnp.clip(jnp.exp(math.log(2.0) - 2.3025851 * jax.random.uniform(key_list[10], (NX2, NY2, LINE), jnp.float32) ** level_of(key_list[10], (NX2, NY2, LINE), ((0, 8), (1, 4)), -0.2, 0.2)), 0.2, 2.0)
    shift_fourth = jnp.clip(jnp.exp(math.log(2.0) - 2.3025851 * jax.random.uniform(key_list[11], (NX3, NY3, LINE), jnp.float32) ** level_of(key_list[11], (NX3, NY3, LINE), ((0, 8), (1, 4)), -0.2, 0.2)), 0.2, 2.0)
    blocks_first = centred(key_list[12], (NX0, NY0, LINKS, LINE, LINE), (LINKS * LINE) ** -0.5, 0.375, ((0, 8), (1, 4)))
    blocks_second = centred(key_list[13], (NX1, NY1, LINKS, LINE, LINE), (LINKS * LINE) ** -0.5, 0.375, ((0, 8), (1, 4)))
    blocks_third = centred(key_list[14], (NX2, NY2, LINKS, LINE, LINE), (LINKS * LINE) ** -0.5, 0.375, ((0, 8), (1, 4)))
    links_first = draw_links_first(jax.random.fold_in(key_list[18], 71), 0)
    links_second = draw_links_second(jax.random.fold_in(key_list[18], 71), 0)
    links_third = draw_links_third(jax.random.fold_in(key_list[18], 71), 0)
    return {"source_first": source_first, "source_second": source_second, "source_third": source_third, "source_fourth": source_fourth, "guess_first": guess_first, "guess_second": guess_second, "guess_third": guess_third, "guess_fourth": guess_fourth, "shift_first": shift_first, "shift_second": shift_second, "shift_third": shift_third, "shift_fourth": shift_fourth, "blocks_first": blocks_first, "blocks_second": blocks_second, "blocks_third": blocks_third, "links_first": links_first, "links_second": links_second, "links_third": links_third}


upper_edge = 14.0
lower_edge = upper_edge / 8.0


def operate(vector, diagonal):
    beside = jnp.roll(vector, 1, 0) + jnp.roll(vector, -1, 0)
    beside = beside + jnp.roll(vector, 1, 1) + jnp.roll(vector, -1, 1)
    beside = beside + jnp.roll(vector, 1, 3) + jnp.roll(vector, -1, 3)
    return (6.0 + diagonal[:, :, None, :]) * vector - beside


def chebyshev(source, initial, diagonal):
    centre = (upper_edge + lower_edge) / 2.0
    half_width = (upper_edge - lower_edge) / 2.0
    ratio_edge = centre / half_width
    factor = 1.0 / ratio_edge
    residual = source - operate(initial, diagonal)
    direction = residual / centre
    result = initial
    for sweep_index in range(DEGREE):
        result = result + direction
        if sweep_index + 1 < DEGREE:
            residual = residual - operate(direction, diagonal)
            factor_next = 1.0 / (2.0 * ratio_edge - factor)
            direction = factor_next * factor * direction + (2.0 * factor_next / half_width) * residual
            factor = factor_next
    return result


def prolong(coarse, link_ids, blocks):
    coarse_lines = coarse.astype(jnp.bfloat16).reshape((-1,) + coarse.shape[2:])

    def one_row(row_pair):
        row_links, row_blocks = row_pair
        picked = coarse_lines[row_links].astype(jnp.float32)
        return jnp.einsum("bkrj,bkij->bri", picked, row_blocks.astype(jnp.float32),
                          precision=lax.Precision.HIGHEST)

    return lax.map(one_row, (link_ids, blocks))


def reference(source_first, source_second, source_third, source_fourth,
              guess_first, guess_second, guess_third, guess_fourth,
              shift_first, shift_second, shift_third, shift_fourth,
              blocks_first, blocks_second, blocks_third,
              links_first, links_second, links_third):
    smooth_fourth = chebyshev(source_fourth, guess_fourth, shift_fourth)
    start_third = guess_third + prolong(smooth_fourth, links_third, blocks_third)
    smooth_third = chebyshev(source_third, start_third, shift_third)
    start_second = guess_second + prolong(smooth_third, links_second, blocks_second)
    smooth_second = chebyshev(source_second, start_second, shift_second)
    start_first = guess_first + prolong(smooth_second, links_first, blocks_first)
    smooth_first = chebyshev(source_first, start_first, shift_first)
    return (smooth_first, smooth_second, smooth_third, smooth_fourth)
```

```python
from functools import partial

import jax
import jax.numpy as jnp
from jax import lax
from jax.experimental import pallas as pl
from jax.experimental.pallas import tpu as pltpu
from jax.sharding import PartitionSpec as P

DEGREE = 3
LEVELS = 4
REACH = DEGREE

upper_edge = 14.0
lower_edge = upper_edge / 8.0


def coefficients():
    centre = (upper_edge + lower_edge) / 2.0
    half_width = (upper_edge - lower_edge) / 2.0
    ratio = centre / half_width
    factor = 1.0 / ratio
    steps = []
    for _ in range(DEGREE - 1):
        following = 1.0 / (2.0 * ratio - factor)
        steps.append((following * factor, 2.0 * following / half_width))
        factor = following
    return 1.0 / centre, steps


def span(offset, length, reach):
    low = max(offset * length, -reach)
    high = min((offset + 1) * length, length + reach)
    return low, high


def plan(nx, ny, reach, box):
    out = []
    far_x, far_y = -(-reach // nx), -(-reach // ny)
    for ox in range(-far_x, far_x + 1):
        for oy in range(-far_y, far_y + 1):
            if ox == 0 and oy == 0:
                continue
            limit = reach - 1 if (ox and oy and not box) else reach
            rows, cols = span(-ox, nx, limit), span(-oy, ny, limit)
            if rows[0] >= rows[1] or cols[0] >= cols[1]:
                continue
            far = (nx * (abs(ox) - 1) + 1 if ox else 0) + (ny * (abs(oy) - 1) + 1 if oy else 0)
            if not box and far > reach:
                continue
            source = (rows[0] + ox * nx, cols[0] + oy * ny)
            out.append((ox, oy, source, (rows[0], cols[0]), (rows[1] - rows[0], cols[1] - cols[0])))
    out.sort(key=lambda m: (abs(m[0]) + abs(m[1]), m))
    return out


def modulo(value, size):
    if size & (size - 1) == 0:
        return jnp.bitwise_and(value, size - 1)
    return lax.rem(value, size)


def quotient(value, size):
    if size & (size - 1) == 0:
        return jnp.right_shift(value, size.bit_length() - 1)
    return lax.div(value, size)


class Counter:
    def __init__(self):
        self.used = 0

    def take(self):
        self.used += 1
        return self.used - 1


def message_count(dims):
    total = 0
    for level, (nx, ny) in enumerate(dims):
        total += len(plan(nx, ny, REACH, False)) + 2 * len(plan(nx, ny, REACH - 1, False))
        if level:
            total += len(plan(nx, ny, 1, True))
    return total


def partners(dims, peers):
    found = set()
    for level, (nx, ny) in enumerate(dims):
        for m in plan(nx, ny, REACH, False) + plan(nx, ny, 1, True):
            found.add((m[0] % peers[0], m[1] % peers[1]))
            found.add((-m[0] % peers[0], -m[1] % peers[1]))
    return sorted(found)


def kernel(dims, peers, *refs):
    sources, guesses, shifts = refs[0:4], refs[4:8], refs[8:12]
    blocks, links = refs[12:15], refs[15:18]
    outs = refs[18:22]
    U, S, D, R, P0, P1, O = (refs[22 + 4 * k : 26 + 4 * k] for k in range(7))
    B, C, H = refs[50:53], refs[53:56], refs[56:60]
    local_sem, send_sem, recv_sem = refs[60:63]
    gz, gy = lax.axis_index("gz"), lax.axis_index("gy")

    def at(ox, oy):
        return (lax.rem(gz + (ox % peers[0]), peers[0]), lax.rem(gy + (oy % peers[1]), peers[1]))

    barrier = pltpu.get_barrier_semaphore()
    company = partners(dims, peers)
    for ox, oy in company:
        pl.semaphore_signal(barrier, inc=1, device_id=at(ox, oy), device_id_type=pl.DeviceIdType.MESH)

    local = Counter()

    def fetch(source, target):
        copy = pltpu.make_async_copy(source, target, local_sem.at[local.take()])
        copy.start()
        return copy

    def own(ref, level, reach):
        nx, ny = dims[level]
        return ref.at[pl.ds(reach, nx), pl.ds(reach, ny)]

    loads = [None] * LEVELS
    for level in reversed(range(LEVELS)):
        loads[level] = [
            fetch(shifts[level], H[level]),
            fetch(guesses[level], own(U[level], level, REACH)),
            fetch(sources[level], own(S[level], level, REACH - 1)),
        ]
    block_loads = [None] * (LEVELS - 1)
    for level in reversed(range(LEVELS - 1)):
        block_loads[level] = fetch(blocks[level], B[level])

    for level in reversed(range(LEVELS)):
        nx, ny = dims[level]
        for copy in loads[level]:
            copy.wait()
        for i in range(nx):
            for j in range(ny):
                D[level][i + REACH - 1, j + REACH - 1] = 6.0 + H[level][i, pl.ds(j, 1)]

    pl.semaphore_wait(barrier, len(company))

    counter = Counter()
    pending = []

    def exchange(ref, level, reach, box=False):
        copies = []
        for ox, oy, source, target, size in plan(*dims[level], reach, box):
            index = counter.take()
            copy = pltpu.make_async_remote_copy(
                src_ref=ref.at[pl.ds(source[0] + reach, size[0]), pl.ds(source[1] + reach, size[1])],
                dst_ref=ref.at[pl.ds(target[0] + reach, size[0]), pl.ds(target[1] + reach, size[1])],
                send_sem=send_sem.at[index],
                recv_sem=recv_sem.at[index],
                device_id=at(ox, oy),
                device_id_type=pl.DeviceIdType.MESH,
            )
            copy.start()
            copies.append(copy)
        pending.extend(copies)
        return copies

    first, steps = coefficients()

    def rows(count, body):
        if count <= 5:
            for i in range(count):
                body(i)
        else:
            lax.fori_loop(0, count, lambda i, c: (body(i), c)[1], 0)

    def operate(ref, diagonal, i, count):
        wide = ref[i + 1]
        middle = wide[1 : count + 1]
        beside = wide[0:count] + wide[2 : count + 2]
        beside = beside + (ref[i, pl.ds(1, count)] + ref[i + 2, pl.ds(1, count)])
        beside = beside + (pltpu.roll(middle, 1, 2) + pltpu.roll(middle, middle.shape[2] - 1, 2))
        return diagonal * middle - beside

    def smooth(level):
        nx, ny = dims[level]
        u, s, d, r, p0, p1, o = (x[level] for x in (U, S, D, R, P0, P1, O))

        def start(i):
            residual = s[i] - operate(u, d[i], i, ny + 4)
            r[i] = residual
            p0[i] = residual * first

        rows(nx + 4, start)
        ahead, along = steps[0]

        def second(i):
            residual = r[i + 1, pl.ds(1, ny + 2)] - operate(p0, d[i + 1, pl.ds(1, ny + 2)], i, ny + 2)
            r[i + 1, pl.ds(1, ny + 2)] = residual
            p1[i] = ahead * p0[i + 1, pl.ds(1, ny + 2)] + along * residual

        rows(nx + 2, second)
        again, around = steps[1]

        def third(i):
            residual = r[i + 2, pl.ds(2, ny)] - operate(p1, d[i + 2, pl.ds(2, ny)], i, ny)
            direction = p1[i + 1, pl.ds(1, ny)]
            last = again * direction + around * residual
            result = u[i + 3, pl.ds(3, ny)] + p0[i + 2, pl.ds(2, ny)] + direction + last
            o[i] = result
            if level:
                C[level - 1][i + 1, pl.ds(1, ny)] = result.astype(jnp.bfloat16)

        rows(nx, third)
        return fetch(o, outs[level])

    def prolong(level):
        nx, ny = dims[level]
        cx, cy = dims[level + 1]
        full = (cx * peers[0], cy * peers[1])
        lift_x = full[0] + 1 - gz * cx
        lift_y = full[1] + 1 - gy * cy

        def pick(i, j, k):
            link = links[level][i, j, k]
            row = modulo(quotient(link, full[1]) + lift_x, full[0])
            col = modulo(modulo(link, full[1]) + lift_y, full[1])
            return C[level][jnp.minimum(row, cx + 1), jnp.minimum(col, cy + 1)]

        def body(i):
            for j in range(ny):
                picked = jnp.concatenate([pick(i, j, 0), pick(i, j, 1)], axis=1)
                block = jnp.concatenate([B[level][i, j, 0], B[level][i, j, 1]], axis=1)
                sums = lax.dot_general(
                    picked, block, (((1,), (1,)), ((), ())), preferred_element_type=jnp.float32
                )
                U[level][i + REACH, j + REACH] = U[level][i + REACH, j + REACH] + sums

        rows(nx, body)

    ready = exchange(U[3], 3, REACH)
    sides = [None] * LEVELS
    for level in reversed(range(LEVELS)):
        sides[level] = exchange(S[level], level, REACH - 1) + exchange(D[level], level, REACH - 1)
    stores = []
    for level in reversed(range(LEVELS)):
        if level < LEVELS - 1:
            block_loads[level].wait()
            prolong(level)
            ready = exchange(U[level], level, REACH)
        for copy in ready + sides[level]:
            copy.wait_recv()
        stores.append(smooth(level))
        if level:
            for copy in exchange(C[level - 1], level, 1, True):
                copy.wait_recv()
    for copy in pending:
        copy.wait_send()
    for copy in stores:
        copy.wait()


def shards(peers, *args):
    dims = [x.shape[:2] for x in args[:4]]
    line = args[0].shape[2:]
    width = line[1:]

    def level_scratch(extra, shape):
        return [pltpu.VMEM((nx + extra, ny + extra) + shape, jnp.float32) for nx, ny in dims]

    scratch = (
        level_scratch(2 * REACH, line)
        + level_scratch(2 * REACH - 2, line)
        + level_scratch(2 * REACH - 2, (1,) + width)
        + level_scratch(2 * REACH - 2, line)
        + level_scratch(2 * REACH - 2, line)
        + level_scratch(2 * REACH - 4, line)
        + level_scratch(0, line)
        + [pltpu.VMEM(x.shape, x.dtype) for x in args[12:15]]
        + [pltpu.VMEM((nx + 2, ny + 2) + line, jnp.bfloat16) for nx, ny in dims[1:]]
        + level_scratch(0, width)
    )
    messages = message_count(dims)
    scratch += [
        pltpu.SemaphoreType.DMA((24,)),
        pltpu.SemaphoreType.DMA((messages,)),
        pltpu.SemaphoreType.DMA((messages,)),
    ]
    anywhere = pl.BlockSpec(memory_space=pl.ANY)
    outs = pl.pallas_call(
        partial(kernel, dims, peers),
        out_shape=[jax.ShapeDtypeStruct(x.shape, x.dtype) for x in args[:4]],
        in_specs=[anywhere] * 15 + [pl.BlockSpec(memory_space=pltpu.SMEM)] * 3,
        out_specs=[anywhere] * 4,
        scratch_shapes=scratch,
        compiler_params=pltpu.CompilerParams(
            collective_id=0, has_side_effects=True, vmem_limit_bytes=40 * 1024 * 1024
        ),
    )(*args)
    return tuple(outs)


def solution(mesh):
    peers = (mesh.shape["gz"], mesh.shape["gy"])
    grid = P("gz", "gy")
    return jax.shard_map(
        partial(shards, peers),
        mesh=mesh,
        in_specs=(grid,) * 18,
        out_specs=(grid,) * 4,
        check_vma=False,
    )
```

```python
from functools import partial

import jax
import jax.numpy as jnp
from jax import lax
from jax.experimental import pallas as pl
from jax.experimental.pallas import tpu as pltpu
from jax.sharding import PartitionSpec as P

DEGREE = 3
LEVELS = 4
REACH = DEGREE

upper_edge = 14.0
lower_edge = upper_edge / 8.0


def coefficients():
    centre = (upper_edge + lower_edge) / 2.0
    half_width = (upper_edge - lower_edge) / 2.0
    ratio = centre / half_width
    factor = 1.0 / ratio
    steps = []
    for _ in range(DEGREE - 1):
        following = 1.0 / (2.0 * ratio - factor)
        steps.append((following * factor, 2.0 * following / half_width))
        factor = following
    return 1.0 / centre, steps


def span(offset, length, reach):
    low = max(offset * length, -reach)
    high = min((offset + 1) * length, length + reach)
    return low, high


def plan(nx, ny, reach, box):
    out = []
    far_x, far_y = -(-reach // nx), -(-reach // ny)
    for ox in range(-far_x, far_x + 1):
        for oy in range(-far_y, far_y + 1):
            if ox == 0 and oy == 0:
                continue
            limit = reach - 1 if (ox and oy and not box) else reach
            rows, cols = span(-ox, nx, limit), span(-oy, ny, limit)
            if rows[0] >= rows[1] or cols[0] >= cols[1]:
                continue
            far = (nx * (abs(ox) - 1) + 1 if ox else 0) + (ny * (abs(oy) - 1) + 1 if oy else 0)
            if not box and far > reach:
                continue
            source = (rows[0] + ox * nx, cols[0] + oy * ny)
            out.append((ox, oy, source, (rows[0], cols[0]), (rows[1] - rows[0], cols[1] - cols[0])))
    out.sort(key=lambda m: (abs(m[0]) + abs(m[1]), m))
    return out


def modulo(value, size):
    if size & (size - 1) == 0:
        return jnp.bitwise_and(value, size - 1)
    return lax.rem(value, size)


def quotient(value, size):
    if size & (size - 1) == 0:
        return jnp.right_shift(value, size.bit_length() - 1)
    return lax.div(value, size)


class Counter:
    def __init__(self):
        self.used = 0

    def take(self):
        self.used += 1
        return self.used - 1


def message_count(dims):
    total = 0
    for level, (nx, ny) in enumerate(dims):
        total += len(plan(nx, ny, REACH, False)) + 2 * len(plan(nx, ny, REACH - 1, False))
        if level:
            total += len(plan(nx, ny, 1, True))
    return total


def partners(dims, peers):
    found = set()
    for level, (nx, ny) in enumerate(dims):
        for m in plan(nx, ny, REACH, False) + plan(nx, ny, 1, True):
            found.add((m[0] % peers[0], m[1] % peers[1]))
            found.add((-m[0] % peers[0], -m[1] % peers[1]))
    return sorted(found)


def kernel(dims, peers, *refs):
    sources, guesses, shifts = refs[0:4], refs[4:8], refs[8:12]
    blocks, links = refs[12:15], refs[15:18]
    outs = refs[18:22]
    U, S, D, R, P0, P1, O = (refs[22 + 4 * k : 26 + 4 * k] for k in range(7))
    B, C, H = refs[50:53], refs[53:56], refs[56:60]
    local_sem, send_sem, recv_sem = refs[60:63]
    gz, gy = lax.axis_index("gz"), lax.axis_index("gy")

    def at(ox, oy):
        return (lax.rem(gz + (ox % peers[0]), peers[0]), lax.rem(gy + (oy % peers[1]), peers[1]))

    barrier = pltpu.get_barrier_semaphore()
    company = partners(dims, peers)
    for ox, oy in company:
        pl.semaphore_signal(barrier, inc=1, device_id=at(ox, oy), device_id_type=pl.DeviceIdType.MESH)

    local = Counter()

    def fetch(source, target):
        copy = pltpu.make_async_copy(source, target, local_sem.at[local.take()])
        copy.start()
        return copy

    def own(ref, level, reach):
        nx, ny = dims[level]
        return ref.at[pl.ds(reach, nx), pl.ds(reach, ny)]

    loads = [None] * LEVELS
    for level in reversed(range(LEVELS)):
        loads[level] = [
            fetch(shifts[level], H[level]),
            fetch(guesses[level], own(U[level], level, REACH)),
            fetch(sources[level], own(S[level], level, REACH - 1)),
        ]
    block_loads = [None] * (LEVELS - 1)
    for level in reversed(range(LEVELS - 1)):
        block_loads[level] = fetch(blocks[level], B[level])

    for level in reversed(range(LEVELS)):
        nx, ny = dims[level]
        for copy in loads[level]:
            copy.wait()
        for i in range(nx):
            for j in range(ny):
                D[level][i + REACH - 1, j + REACH - 1] = 6.0 + H[level][i, pl.ds(j, 1)]

    pl.semaphore_wait(barrier, len(company))

    counter = Counter()
    pending = []

    def exchange(ref, level, reach, box=False):
        copies = []
        for ox, oy, source, target, size in plan(*dims[level], reach, box):
            index = counter.take()
            copy = pltpu.make_async_remote_copy(
                src_ref=ref.at[pl.ds(source[0] + reach, size[0]), pl.ds(source[1] + reach, size[1])],
                dst_ref=ref.at[pl.ds(target[0] + reach, size[0]), pl.ds(target[1] + reach, size[1])],
                send_sem=send_sem.at[index],
                recv_sem=recv_sem.at[index],
                device_id=at(ox, oy),
                device_id_type=pl.DeviceIdType.MESH,
            )
            copy.start()
            copies.append(copy)
        pending.extend(copies)
        return copies

    first, steps = coefficients()

    def rows(count, body):
        if count <= 5:
            for i in range(count):
                body(i)
        else:
            lax.fori_loop(0, count, lambda i, c: (body(i), c)[1], 0)

    def operate(ref, diagonal, i, count):
        wide = ref[i + 1]
        middle = wide[1 : count + 1]
        beside = wide[0:count] + wide[2 : count + 2]
        beside = beside + (ref[i, pl.ds(1, count)] + ref[i + 2, pl.ds(1, count)])
        beside = beside + (pltpu.roll(middle, 1, 2) + pltpu.roll(middle, middle.shape[2] - 1, 2))
        return diagonal * middle - beside

    def smooth(level):
        nx, ny = dims[level]
        u, s, d, r, p0, p1, o = (x[level] for x in (U, S, D, R, P0, P1, O))

        def start(i):
            residual = s[i] - operate(u, d[i], i, ny + 4)
            r[i] = residual
            p0[i] = residual * first

        rows(nx + 4, start)
        ahead, along = steps[0]

        def second(i):
            residual = r[i + 1, pl.ds(1, ny + 2)] - operate(p0, d[i + 1, pl.ds(1, ny + 2)], i, ny + 2)
            r[i + 1, pl.ds(1, ny + 2)] = residual
            p1[i] = ahead * p0[i + 1, pl.ds(1, ny + 2)] + along * residual

        rows(nx + 2, second)
        again, around = steps[1]

        def third(i):
            residual = r[i + 2, pl.ds(2, ny)] - operate(p1, d[i + 2, pl.ds(2, ny)], i, ny)
            direction = p1[i + 1, pl.ds(1, ny)]
            last = again * direction + around * residual
            result = u[i + 3, pl.ds(3, ny)] + p0[i + 2, pl.ds(2, ny)] + direction + last
            o[i] = result
            if level:
                C[level - 1][i + 1, pl.ds(1, ny)] = result.astype(jnp.bfloat16)

        rows(nx, third)
        return fetch(o, outs[level])

    def prolong(level):
        nx, ny = dims[level]
        cx, cy = dims[level + 1]
        full = (cx * peers[0], cy * peers[1])
        lift_x = full[0] + 1 - gz * cx
        lift_y = full[1] + 1 - gy * cy

        def pick(i, j, k):
            link = links[level][i, j, k]
            row = modulo(quotient(link, full[1]) + lift_x, full[0])
            col = modulo(modulo(link, full[1]) + lift_y, full[1])
            return C[level][jnp.minimum(row, cx + 1), jnp.minimum(col, cy + 1)]

        def body(i):
            for j in range(ny):
                picked = jnp.concatenate([pick(i, j, 0), pick(i, j, 1)], axis=1)
                block = jnp.concatenate([B[level][i, j, 0], B[level][i, j, 1]], axis=1)
                sums = lax.dot_general(
                    picked, block, (((1,), (1,)), ((), ())), preferred_element_type=jnp.float32
                )
                U[level][i + REACH, j + REACH] = U[level][i + REACH, j + REACH] + sums

        rows(nx, body)

    ready = exchange(U[3], 3, REACH)
    sides = [None] * LEVELS
    for level in reversed(range(1, LEVELS)):
        sides[level] = exchange(S[level], level, REACH - 1) + exchange(D[level], level, REACH - 1)
    stores = []
    for level in reversed(range(LEVELS)):
        if level < LEVELS - 1:
            block_loads[level].wait()
            prolong(level)
            ready = exchange(U[level], level, REACH)
        for copy in ready + sides[level]:
            copy.wait_recv()
        if level == 2:
            sides[0] = exchange(S[0], 0, REACH - 1) + exchange(D[0], 0, REACH - 1)
        stores.append(smooth(level))
        if level:
            for copy in exchange(C[level - 1], level, 1, True):
                copy.wait_recv()
    for copy in pending:
        copy.wait_send()
    for copy in stores:
        copy.wait()


def shards(peers, *args):
    dims = [x.shape[:2] for x in args[:4]]
    line = args[0].shape[2:]
    width = line[1:]

    def level_scratch(extra, shape):
        return [pltpu.VMEM((nx + extra, ny + extra) + shape, jnp.float32) for nx, ny in dims]

    scratch = (
        level_scratch(2 * REACH, line)
        + level_scratch(2 * REACH - 2, line)
        + level_scratch(2 * REACH - 2, (1,) + width)
        + level_scratch(2 * REACH - 2, line)
        + level_scratch(2 * REACH - 2, line)
        + level_scratch(2 * REACH - 4, line)
        + level_scratch(0, line)
        + [pltpu.VMEM(x.shape, x.dtype) for x in args[12:15]]
        + [pltpu.VMEM((nx + 2, ny + 2) + line, jnp.bfloat16) for nx, ny in dims[1:]]
        + level_scratch(0, width)
    )
    messages = message_count(dims)
    scratch += [
        pltpu.SemaphoreType.DMA((24,)),
        pltpu.SemaphoreType.DMA((messages,)),
        pltpu.SemaphoreType.DMA((messages,)),
    ]
    anywhere = pl.BlockSpec(memory_space=pl.ANY)
    outs = pl.pallas_call(
        partial(kernel, dims, peers),
        out_shape=[jax.ShapeDtypeStruct(x.shape, x.dtype) for x in args[:4]],
        in_specs=[anywhere] * 15 + [pl.BlockSpec(memory_space=pltpu.SMEM)] * 3,
        out_specs=[anywhere] * 4,
        scratch_shapes=scratch,
        compiler_params=pltpu.CompilerParams(
            collective_id=0, has_side_effects=True, vmem_limit_bytes=67043328
        ),
    )(*args)
    return tuple(outs)


def solution(mesh):
    peers = (mesh.shape["gz"], mesh.shape["gy"])
    grid = P("gz", "gy")
    return jax.shard_map(
        partial(shards, peers),
        mesh=mesh,
        in_specs=(grid,) * 18,
        out_specs=(grid,) * 4,
        check_vma=False,
    )
```
